32 devices in a mesh: band: 2 (over x), vis: 16 (over z, y, core).
Axes of the slice: x: 2, y: 2, z: 4, core: 2. Of those that a mesh axis runs over, the one named last changes fastest.
Arguments:
- sky_image: float32 [4096, 4096], P(('band', 'vis')), as said below
- coef_dual: float32 [4, 2048, 2048], P(None, ('band', 'vis')), may hold values from -12 to 12
- vis_dual: float32 [2, 16, 16, 4, 2, 32], P('band', 'vis'), may hold values from -12 to 12
- visibilities: float32 [2, 16, 16, 4, 2, 32], P('band', 'vis')
- kernel_blocks: bfloat16 [2, 16, 16, 4, 2, 32, 256], P('band', 'vis'), may hold values from -0.375 to 0.375
- tile_rows: int32 [2, 16, 16, 4], P('band', 'vis'), may hold values from 0 to 2047
- tile_counts: int32 [2, 16, 16], P('band', 'vis'), may hold values from 1 to 4, as said below
Outputs:
- new_image: float32 [4096, 4096], P(('band', 'vis'))
- new_coef_dual: float32 [4, 2048, 2048], P(None, ('band', 'vis'))
- new_vis_dual: float32 [2, 16, 16, 4, 2, 32], P('band', 'vis')
The draws below stay inside these ranges and needn't reach their ends.
Inputs may be any that keep to these rules, and one draw needn't show every extreme that they name: `sky_image`: nonnegative. `tile_counts`: in every band some owner q has all 4 slots live from every device of that band.
All inputs are finite; a program needn't handle non-finite values.
Results may differ from the reference program's by a relative error of at most 0.0018.
Values may be sent and summed in bfloat16 or wider, within the bound.
No kernel may reach another device: no remote copies, remote signals or barrier semaphores. Data moves between devices by JAX's collectives and lax.ppermute only.
A program may use at most 128 MiB of HBM per device.

```python
import jax
import jax.numpy as jnp
from jax import lax

IMG = 4096
VT = 32
SLOTS = 4
ITERS = 1
STRIPE = 2048
PIECE_ROWS = 256
HALF = 2048
N_BAND = 2
N_VIS = 16


def draw_sky_image(key, part):
    row_key, col_key, base_key = jax.random.split(key, 3)
    row_scale = jnp.exp(jax.random.uniform(row_key, (IMG, 1), jnp.float32) * jnp.log(10.0))
    col_scale = jnp.exp(jax.random.uniform(col_key, (1, IMG), jnp.float32) * jnp.log(10.0))
    rising = 1.0 + 2.0 * jnp.arange(IMG, dtype=jnp.float32)[:, None] / IMG
    base_values = jax.random.uniform(base_key, (IMG, IMG), jnp.float32)
    return 0.2 * base_values * row_scale * col_scale * rising


def draw_visibilities(key, part):
    full_shape = (N_BAND, N_VIS, N_VIS, SLOTS, 2, VT)
    scale_key, value_key = jax.random.split(key)
    tile_scale = jnp.exp(jax.random.uniform(scale_key, (N_BAND, N_VIS, N_VIS, SLOTS, 1, 1), jnp.float32) * jnp.log(10.0))
    position = (jnp.arange(N_BAND * N_VIS, dtype=jnp.float32) / (N_BAND * N_VIS - 1)).reshape(N_BAND, N_VIS, 1, 1, 1, 1)
    values = jax.random.normal(value_key, full_shape, jnp.float32)
    rising = 1.0 + 2.0 * position
    return values * tile_scale * rising


def draw_tile_counts(key, part):
    count_key, owner_key = jax.random.split(jax.random.fold_in(key, 11))
    counts = jax.random.randint(count_key, (N_BAND, N_VIS, N_VIS), 1, SLOTS + 1)
    full_owner = jax.random.randint(owner_key, (N_BAND, 1, 1), 0, N_VIS)
    owners = jnp.arange(N_VIS, dtype=jnp.int32)[None, None, :]
    return jnp.where(owners == full_owner, SLOTS, counts).astype(jnp.int32)


def plant(values, key, low, largest):
    extent = values.shape
    spot = [jax.random.randint(jax.random.fold_in(key, axis), (), 0, extent[axis]) for axis in range(len(extent))]
    values = values.at[tuple(spot)].set(low)
    longest = extent.index(max(extent))
    spot[longest] = (spot[longest] + 1) % extent[longest]
    return values.at[tuple(spot)].set(largest)


def block_levels(rng, shape, cuts, least, largest):
    loudness, own = 1.0, jax.random.fold_in(rng, 6)
    for dim, shards_of in cuts:
        heights = jnp.exp(jax.random.uniform(jax.random.fold_in(own, dim), (shards_of,), jnp.float32, least / len(cuts), largest / len(cuts)))
        loudness = loudness * jnp.repeat(heights, shape[dim] // shards_of).reshape([-1 if axis == dim else 1 for axis in range(len(shape))])
    return loudness


def centred(own_key, extent, width, limit, cuts=(), held_as=jnp.bfloat16):
    entries = width * jax.random.normal(own_key, extent, jnp.float32)
    if cuts:
        entries = entries * block_levels(own_key, extent, cuts, -0.22, 0.18)
    return jnp.clip(entries, -limit, limit).astype(held_as)


def setup_inputs(seed: int = 0) -> dict:
    splits = jax.random.split(jax.random.key(seed), 8)
    sky_image = draw_sky_image(jax.random.fold_in(splits[7], 71), 0)
    coef_dual = centred(splits[1], (4, HALF, HALF), 2.0, 12.0, ((1, 32),), jnp.float32)
    vis_dual = centred(splits[2], (N_BAND, N_VIS, N_VIS, SLOTS, 2, VT), 2.0, 12.0, ((0, 2), (1, 16)), jnp.float32)
    visibilities = draw_visibilities(jax.random.fold_in(splits[7], 71), 0)
    kernel_blocks = centred(splits[4], (N_BAND, N_VIS, N_VIS, SLOTS, 2, VT, PIECE_ROWS), PIECE_ROWS ** -0.5, 0.375, ((0, 2), (1, 16)))
    tile_rows = plant(jax.random.randint(splits[5], (N_BAND, N_VIS, N_VIS, SLOTS), 0, STRIPE), jax.random.fold_in(splits[5], 1), 0, STRIPE - 1).astype(jnp.int32)
    tile_counts = draw_tile_counts(jax.random.fold_in(splits[7], 71), 0)
    return dict(sky_image=sky_image, coef_dual=coef_dual, vis_dual=vis_dual, visibilities=visibilities, kernel_blocks=kernel_blocks, tile_rows=tile_rows, tile_counts=tile_counts)


low_taps = (-0.010597401784997278, 0.032883011666982945, 0.030841381835986965, -0.18703481171888114, -0.02798376941698385, 0.6308807679295904, 0.7148465705525415, 0.23037781330885523)
high_taps = tuple(((-1.0) ** offset * low_taps[7 - offset] for offset in range(8)))
highest = lax.Precision.HIGHEST

def analyse_axis(field, axis):
    length = field.shape[axis]
    low_part = 0.0
    high_part = 0.0
    for offset in range(8):
        taken = lax.slice_in_dim(jnp.roll(field, -offset, axis=axis), 0, length, 2, axis)
        low_part = low_part + low_taps[offset] * taken
        high_part = high_part + high_taps[offset] * taken
    return (low_part, high_part)

def synthesise_axis(low_part, high_part, axis):
    halves = []
    for parity in range(2):
        summed = 0.0
        for delay in range(4):
            summed = summed + low_taps[parity + 2 * delay] * jnp.roll(low_part, delay, axis=axis)
            summed = summed + high_taps[parity + 2 * delay] * jnp.roll(high_part, delay, axis=axis)
        halves.append(summed)
    joined = jnp.stack(halves, axis=axis + 1)
    new_shape = list(low_part.shape)
    new_shape[axis] = 2 * new_shape[axis]
    return joined.reshape(new_shape)

def analysis(field):
    rows_low, rows_high = analyse_axis(field, 0)
    low_low, low_high = analyse_axis(rows_low, 1)
    high_low, high_high = analyse_axis(rows_high, 1)
    return jnp.stack([low_low, low_high, high_low, high_high])

def synthesis(coeffs):
    rows_low = synthesise_axis(coeffs[0], coeffs[1], 1)
    rows_high = synthesise_axis(coeffs[2], coeffs[3], 1)
    return synthesise_axis(rows_low, rows_high, 0)

def forward_map(extrap, kernel_blocks, tile_rows):
    spectrum = jnp.fft.fft2(extrap) / IMG
    flipped = spectrum.T.reshape(N_BAND, STRIPE, N_VIS, PIECE_ROWS)
    real_grid = lax.optimization_barrier(jnp.real(flipped).astype(jnp.bfloat16))
    imag_grid = lax.optimization_barrier(jnp.imag(flipped).astype(jnp.bfloat16))
    owners = jnp.arange(N_VIS, dtype=jnp.int32)[None, :, None]

    def per_band(inputs):
        kernels, rows_band, real_band, imag_band = inputs
        tile_real = real_band[rows_band, owners].astype(jnp.float32)
        tile_imag = imag_band[rows_band, owners].astype(jnp.float32)
        kernel_real = kernels[:, :, :, 0].astype(jnp.float32)
        kernel_imag = kernels[:, :, :, 1].astype(jnp.float32)
        out_real = jnp.einsum('vqsat,vqst->vqsa', kernel_real, tile_real, precision=highest) - jnp.einsum('vqsat,vqst->vqsa', kernel_imag, tile_imag, precision=highest)
        out_imag = jnp.einsum('vqsat,vqst->vqsa', kernel_real, tile_imag, precision=highest) + jnp.einsum('vqsat,vqst->vqsa', kernel_imag, tile_real, precision=highest)
        return jnp.stack([out_real, out_imag], axis=3)
    return lax.map(per_band, (kernel_blocks, tile_rows, real_grid, imag_grid))

def adjoint_map(weights, kernel_blocks, tile_rows):
    rounded = lax.optimization_barrier(weights.astype(jnp.bfloat16))
    owners = jnp.arange(N_VIS, dtype=jnp.int32)[None, :, None]

    def per_band(inputs):
        kernels, rows_band, vis_band = inputs
        kernel_real = kernels[:, :, :, 0].astype(jnp.float32)
        kernel_imag = kernels[:, :, :, 1].astype(jnp.float32)
        weight_real = vis_band[:, :, :, 0].astype(jnp.float32)
        weight_imag = vis_band[:, :, :, 1].astype(jnp.float32)
        grid_real = jnp.einsum('vqsat,vqsa->vqst', kernel_real, weight_real, precision=highest) + jnp.einsum('vqsat,vqsa->vqst', kernel_imag, weight_imag, precision=highest)
        grid_imag = jnp.einsum('vqsat,vqsa->vqst', kernel_real, weight_imag, precision=highest) - jnp.einsum('vqsat,vqsa->vqst', kernel_imag, weight_real, precision=highest)
        stacked = jnp.stack([grid_real, grid_imag], axis=3)
        segment = (owners * STRIPE + rows_band).astype(jnp.int32)
        summed = jax.ops.segment_sum(stacked.reshape(-1, 2, PIECE_ROWS), segment.reshape(-1), num_segments=N_VIS * STRIPE)
        return summed.reshape(N_VIS, STRIPE, 2, PIECE_ROWS)
    grids = lax.map(per_band, (kernel_blocks, tile_rows, rounded))
    ordered = jnp.transpose(grids, (3, 1, 4, 0, 2)).reshape(2, IMG, IMG)
    spectrum = lax.complex(ordered[0], ordered[1])
    return jnp.real(jnp.fft.ifft2(spectrum)) * IMG

def reference(sky_image, coef_dual, vis_dual, visibilities, kernel_blocks, tile_rows, tile_counts):
    slot_index = jnp.arange(SLOTS, dtype=jnp.int32)
    live_slots = (slot_index < tile_counts[..., None]).astype(jnp.float32)[..., None, None]
    data_square = jnp.sum(live_slots * visibilities * visibilities)
    radius = 0.5 * jnp.sqrt(data_square + 1e-06)
    for iteration in range(ITERS):
        adjoint_part = adjoint_map(live_slots * vis_dual, kernel_blocks, tile_rows)
        smooth = synthesis(coef_dual)
        new_image = jnp.maximum(sky_image - smooth - adjoint_part, 0.0)
        extrap = 2.0 * new_image - sky_image
        coeffs = analysis(extrap)
        threshold = 0.5 * jnp.sum(jnp.abs(coeffs)) / (IMG * IMG)
        coef_dual = jnp.clip(coef_dual + coeffs, -threshold, threshold)
        predicted = forward_map(extrap, kernel_blocks, tile_rows)
        residual = live_slots * (vis_dual + predicted - visibilities)
        size_value = jnp.sqrt(jnp.sum(residual * residual) + 1e-06)
        vis_dual = residual * (1.0 - jnp.minimum(1.0, radius / size_value))
        sky_image = new_image
    return (sky_image, coef_dual, vis_dual)
```

```python
import math

import jax
import jax.numpy as jnp
import numpy as np
from jax import lax
from jax.experimental import pallas as pl
from jax.experimental.pallas import tpu as pltpu
from jax.sharding import PartitionSpec as P

LANES = 128
FLAG = 1 << 20

low_taps = (
    -0.010597401784997278,
    0.032883011666982945,
    0.030841381835986965,
    -0.18703481171888114,
    -0.02798376941698385,
    0.6308807679295904,
    0.7148465705525415,
    0.23037781330885523,
)
high_taps = tuple(((-1.0) ** offset * low_taps[7 - offset] for offset in range(8)))
AXES = ("band", "vis")
bf16 = jnp.bfloat16
f32 = jnp.float32


def shifted(block, axis, distance):
    devices = range(lax.axis_size(axis))
    route = [((i - distance) % len(devices), i) for i in devices]
    return lax.ppermute(block, axis, route)


def flipped(block, axis, mask):
    return lax.ppermute(block, axis, [(i, i ^ mask) for i in range(lax.axis_size(axis))])


def split_two(values):
    high = lax.reduce_precision(values, 8, 7)
    return high.astype(bf16), (values - high).astype(bf16)


def split_here(values):
    high = values.astype(bf16)
    return high, (values - high.astype(f32)).astype(bf16)


def dot_nn(left, right):
    return lax.dot_general(left, right, (((1,), (0,)), ((), ())), preferred_element_type=f32)


def dot_nt(left, right):
    return lax.dot_general(left, right, (((1,), (1,)), ((), ())), preferred_element_type=f32)


def dot_three(dot, left, right):
    return dot(left[0], right[0]) + dot(left[0], right[1]) + dot(left[1], right[0])


def scaled_sum(terms):
    total = None
    for weight, value in terms:
        if abs(weight) < 1e-12:
            continue
        part = value if weight == 1.0 else weight * value
        total = part if total is None else total + part
    return total


def cosine_sums(values, size):
    if size == 1:
        return [values[0] + values[1], values[0] - values[1]]
    half = size // 2
    even = cosine_sums(values[0::2], half)
    out = [None] * (size + 1)
    for a in range(half):
        odd = scaled_sum(
            [(math.cos(math.pi * k * a / size) if a else 1.0, values[k]) for k in range(1, size, 2)]
        )
        out[a] = even[a] + odd
        out[size - a] = even[a] - odd
    out[half] = even[half]
    return out


def sine_sums(values, size):
    half = size // 2
    out = [None] * (size + 1)
    if size == 2:
        out[1] = values[1]
        return out
    even = sine_sums(values[0::2], half)
    for a in range(1, half):
        odd = scaled_sum([(math.sin(math.pi * k * a / size), values[k]) for k in range(1, size, 2)])
        out[a] = odd + even[a]
        out[size - a] = odd - even[a]
    out[half] = scaled_sum([(math.sin(math.pi * k / 2), values[k]) for k in range(1, size, 2)])
    return out


def twiddle_seeds(image_width):
    outer = image_width // LANES
    kept = outer // 2 + 1
    inner = image_width // outer
    c = np.arange(LANES)
    one = 2.0 * np.pi * (np.arange(kept)[:, None] * c[None, :] % image_width) / image_width
    two = 2.0 * np.pi * (np.arange(inner)[:, None] * c[None, :] % inner) / inner
    one = np.stack([np.cos(one), np.sin(one)], axis=1).astype(np.float32)
    two = np.stack([np.cos(two), np.sin(two)]).astype(np.float32)
    return jnp.asarray(one), jnp.asarray(two)


def upright(row):
    return jnp.broadcast_to(row, (8, row.shape[1])).T[:, 0:1]


def sign_of(code):
    return jnp.where(code >= FLAG, -1.0, 1.0).astype(f32)


def whole(array):
    return pl.BlockSpec(array.shape, lambda i: (0,) * array.ndim)


def adjoint_map(tile_real, tile_imag, codes, weight_tables, phases, sky_image, smooth):
    blocks_c, blocks_a, blocks_b, blocks_f, tiles, length = tile_real.shape
    blocks_ab = blocks_a * blocks_b
    blocks = blocks_c * blocks_ab * blocks_f
    rows, image_width = sky_image.shape
    outer = image_width // LANES
    kept = outer // 2 + 1
    inner = image_width // outer
    width = kept * inner
    seeds = twiddle_seeds(image_width)
    each = -(-kept // blocks)

    def kernel(
        tre, tim, code_ref, wrh, wrl, wih, wil, pc, ps, one, two, sky, smo,
        new_ref, ext_ref, x_ref, grid_ref, mid_ref, y_ref, mh, ml,
    ):
        step = pl.program_id(0)

        @pl.when(step == 0)
        def _():
            grid_ref[...] = jnp.zeros_like(grid_ref)

        @pl.when(step < blocks)
        def _():
            re = tre[0, 0, 0, 0]
            im = tim[0, 0, 0, 0]
            half = (
                dot_nt(wrh[...], re) + dot_nt(wrl[...], re)
                + dot_nt(wih[...], im) + dot_nt(wil[...], im)
            )
            half_re = half[:rows]
            half_im = half[rows:]
            code = code_ref[0]
            turned_re = pc[...] * half_re - ps[...] * half_im
            turned_im = (pc[...] * half_im + ps[...] * half_re) * sign_of(code)
            turned = jnp.concatenate([turned_re, turned_im], axis=0).astype(bf16)
            column = upright(code & (FLAG - 1))
            lanes = lax.broadcasted_iota(jnp.int32, (tiles, inner), 1)
            within = (lanes == column % inner).astype(f32).astype(bf16)
            major = jnp.broadcast_to((column // inner).astype(f32), (tiles, inner)).astype(bf16)
            zero = jnp.zeros_like(within)
            for begin in range(0, kept, 2):
                hots = [
                    jnp.where(major == jnp.asarray(k, bf16), within, zero)
                    for k in range(begin, min(begin + 2, kept))
                ]
                span = slice(begin * inner, (begin + len(hots)) * inner)
                grid_ref[:, span] += dot_nn(turned, jnp.concatenate(hots, axis=1))
            for u in range(each):
                k = jnp.minimum(step * each + u, kept - 1)
                c1 = one[k, 0:1, :]
                s1 = one[k, 1:2, :]
                c2 = two[0]
                s2 = two[1]
                real = split_here(c1 * c2 - s1 * s2)
                imag = split_here(c1 * s2 + s1 * c2)
                for out, re, im in ((mh, real[0], imag[0]), (ml, real[1], imag[1])):
                    out[k, 0:inner, 0:LANES] = re
                    out[k, 0:inner, LANES : 2 * LANES] = im
                    out[k, inner : 2 * inner, 0:LANES] = -im
                    out[k, inner : 2 * inner, LANES : 2 * LANES] = re

        @pl.when(step == blocks)
        def _():
            for k in range(kept):
                cell = jnp.concatenate(
                    [
                        grid_ref[:rows, k * inner : (k + 1) * inner],
                        grid_ref[rows:, k * inner : (k + 1) * inner],
                    ],
                    axis=1,
                )
                mid_ref[k] = dot_three(dot_nn, split_here(cell), (mh[k], ml[k]))

            def body(chunk, carry):
                at = pl.ds(pl.multiple_of(chunk * 8, 8), 8)
                real = [mid_ref[k, at, 0:LANES] for k in range(kept)]
                imag = [mid_ref[k, at, LANES : 2 * LANES] for k in range(kept)]
                even = cosine_sums(real, outer // 2)
                odd = sine_sums(imag, outer // 2)
                values = []
                for a in range(outer):
                    if a == 0 or a == outer // 2:
                        back = even[a]
                    elif a < outer // 2:
                        back = even[a] - odd[a]
                    else:
                        back = even[outer - a] + odd[outer - a]
                    span = slice(a * LANES, (a + 1) * LANES)
                    old = sky[at, span]
                    new = jnp.maximum(old - smo[at, span] - back, 0.0)
                    extrap = 2.0 * new - old
                    new_ref[at, span] = new
                    ext_ref[at, span] = extrap
                    values.append(extrap)
                mirrored = outer // 2
                even = [values[0]]
                odd = [None]
                for a in range(1, mirrored):
                    even.append(values[a] + values[outer - a])
                    odd.append(values[a] - values[outer - a])
                even.append(values[mirrored])
                odd.append(None)
                real = cosine_sums(even, mirrored)
                imag = sine_sums(odd, mirrored)
                for k in range(kept):
                    y_ref[k, at, 0:LANES] = real[k]
                    y_ref[k, at, LANES : 2 * LANES] = (
                        jnp.zeros_like(real[k]) if imag[k] is None else -imag[k]
                    )
                return carry

            lax.fori_loop(0, rows // 8, body, 0)
            for k in range(kept):
                high, low = split_here(y_ref[k])
                if rows % LANES == 0:
                    both = dot_nt(mh[k], jnp.concatenate([high, low], axis=0))
                    both = both[:, :rows] + both[:, rows:] + dot_nt(ml[k], high)
                else:
                    both = dot_three(dot_nt, (mh[k], ml[k]), (high, low))
                x_ref[k * inner : (k + 1) * inner, :] = jnp.concatenate(
                    [both[:inner], both[inner:]], axis=1
                )

    def tile_block_a(i):
        i = jnp.minimum(i, blocks - 1)
        j, f = i // blocks_f, i % blocks_f
        return (j // blocks_ab, j // blocks_b % blocks_a, j % blocks_b, f, 0, 0)

    def tile_block_b(i):
        c, y, x, f, _, _ = tile_block_a(i)
        return (c, x, y, f, 0, 0)

    image = jax.ShapeDtypeStruct((rows, image_width), f32)
    return pl.pallas_call(
        kernel,
        grid=(blocks + 1,),
        in_specs=[
            pl.BlockSpec((1, 1, 1, 1, tiles, length), tile_block_a),
            pl.BlockSpec((1, 1, 1, 1, tiles, length), tile_block_b),
            pl.BlockSpec((1, 1, tiles), lambda i: (jnp.minimum(i, blocks - 1), 0, 0)),
            *[whole(w) for w in weight_tables],
            *[whole(p) for p in phases],
            *[whole(t) for t in seeds],
            whole(sky_image),
            whole(smooth),
        ],
        out_specs=[
            pl.BlockSpec((rows, image_width), lambda i: (0, 0)),
            pl.BlockSpec((rows, image_width), lambda i: (0, 0)),
            pl.BlockSpec((width, 2 * rows), lambda i: (0, 0)),
        ],
        out_shape=[image, image, jax.ShapeDtypeStruct((width, 2 * rows), f32)],
        scratch_shapes=[
            pltpu.VMEM((2 * rows, width), f32),
            pltpu.VMEM((kept, rows, 2 * LANES), f32),
            pltpu.VMEM((kept, rows, 2 * LANES), f32),
            pltpu.VMEM((kept, 2 * inner, 2 * LANES), bf16),
            pltpu.VMEM((kept, 2 * inner, 2 * LANES), bf16),
        ],
        cost_estimate=pl.CostEstimate(
            flops=8 * blocks * rows * tiles * (width + length), bytes_accessed=1 << 24, transcendentals=0
        ),
        name="adjoint",
    )(tile_real, tile_imag, codes, *weight_tables, *phases, *seeds, sky_image, smooth)


def forward_parts(spectrum, codes, weight_tables, phases, part, counts):
    blocks_a, blocks_b, blocks_f = counts
    blocks = blocks_a * blocks_b * blocks_f
    tiles = codes.shape[2]
    width, rows2 = spectrum.shape
    rows = rows2 // 2
    length = weight_tables[0].shape[1]
    together = 16

    def kernel(x_ref, where, code_ref, wrh, wrl, wih, wil, pc, ps, out_ref, pick_ref):
        def body(chunk, carry):
            begin = chunk * together
            found = [
                x_ref[pl.ds(where[0, 0, begin + u] & (FLAG - 1), 1), :] for u in range(together)
            ]
            for u in range(together):
                pick_ref[pl.ds(begin + u, 1), :] = found[u]
            return carry

        lax.fori_loop(0, tiles // together, body, 0)
        sign = upright(sign_of(code_ref[0]))
        real = pick_ref[:, :rows]
        imag = pick_ref[:, rows:] * sign
        turned_re = pc[...] * real + ps[...] * imag
        turned_im = pc[...] * imag - ps[...] * real
        turned = split_here(jnp.concatenate([turned_re, turned_im], axis=1))
        out_ref[0, 0, 0, 0] = dot_three(dot_nn, turned, (wrh[...], wrl[...]))
        out_ref[1, 0, 0, 0] = dot_three(dot_nn, turned, (wih[...], wil[...]))

    return pl.pallas_call(
        kernel,
        grid=(blocks,),
        in_specs=[
            whole(spectrum),
            pl.BlockSpec((1, 1, tiles), lambda i: (part * blocks + i, 0, 0), memory_space=pltpu.SMEM),
            pl.BlockSpec((1, 1, tiles), lambda i: (part * blocks + i, 0, 0)),
            *[whole(w) for w in weight_tables],
            *[whole(p) for p in phases],
        ],
        out_specs=pl.BlockSpec(
            (2, 1, 1, 1, tiles, length),
            lambda i: (0, i // blocks_f // blocks_b, i // blocks_f % blocks_b, i % blocks_f, 0, 0),
        ),
        out_shape=jax.ShapeDtypeStruct((2, *counts, tiles, length), f32),
        scratch_shapes=[pltpu.VMEM((tiles, 2 * rows), f32)],
        cost_estimate=pl.CostEstimate(
            flops=24 * blocks * rows * tiles * length, bytes_accessed=1 << 23, transcendentals=0
        ),
        name="parts",
    )(spectrum, codes, codes, *weight_tables, *phases)


def row_matrix_up(half_rows, lead):
    ext = half_rows + lead
    matrix = np.zeros((2 * half_rows, 2 * ext), np.float64)
    for n in range(2 * half_rows):
        for k in range(-3, half_rows):
            tap = n - 2 * k
            if 0 <= tap < 8:
                matrix[n, lead + k] = low_taps[tap]
                matrix[n, ext + lead + k] = high_taps[tap]
    return matrix


def row_matrix_down(rows, tail):
    matrix = np.zeros((rows, rows + tail), np.float64)
    for k in range(rows // 2):
        for j in range(8):
            matrix[k, 2 * k + j] = low_taps[j]
            matrix[rows // 2 + k, 2 * k + j] = high_taps[j]
    return matrix


def col_matrix_up():
    matrix = np.zeros((4, LANES, 2 * LANES), np.float64)
    for n in range(2 * LANES):
        for k in range(-LANES, LANES):
            tap = n - 2 * k
            if 0 <= tap < 8:
                where = (0, k + LANES) if k < 0 else (1, k)
                matrix[where[0], where[1], n] = low_taps[tap]
                matrix[2 + where[0], where[1], n] = high_taps[tap]
    return matrix.reshape(4 * LANES, 2 * LANES)


def col_matrix_down():
    matrix = np.zeros((3 * LANES, 2 * LANES), np.float64)
    for k in range(LANES):
        for j in range(8):
            matrix[2 * k + j, k] = low_taps[j]
            matrix[2 * k + j, LANES + k] = high_taps[j]
    return matrix


def split_constant(matrix):
    value = np.asarray(matrix, np.float32)
    high = value.astype(bf16)
    low = (value - high.astype(np.float32)).astype(bf16)
    return jnp.asarray(high), jnp.asarray(low)


def synthesis(halo, coef_dual):
    _, half_rows, half_width = coef_dual.shape
    rows = 2 * half_rows
    lead = halo.shape[1]
    row_tables = split_constant(row_matrix_up(half_rows, lead))
    col_tables = split_constant(col_matrix_up())

    def kernel(halo_ref, coef_ref, rh, rl, ch, cl, out_ref):
        sides = []
        for first, second in ((0, 2), (1, 3)):
            ext = jnp.concatenate(
                [halo_ref[first], coef_ref[first], halo_ref[second], coef_ref[second]], axis=0
            )
            sides.append(dot_three(dot_nn, (rh[...], rl[...]), split_here(ext)))
        low = split_here(sides[0])
        high = split_here(sides[1])
        count = half_width // LANES
        for j in range(count):
            here = slice(j * LANES, (j + 1) * LANES)
            past = (j - 1) % count
            before = slice(past * LANES, (past + 1) * LANES)
            operands = tuple(
                jnp.concatenate(
                    [low[p][:, before], low[p][:, here], high[p][:, before], high[p][:, here]],
                    axis=1,
                )
                for p in range(2)
            )
            out_ref[:, 2 * j * LANES : 2 * (j + 1) * LANES] = dot_three(
                dot_nn, operands, (ch[...], cl[...])
            )

    return pl.pallas_call(
        kernel,
        out_shape=jax.ShapeDtypeStruct((rows, 2 * half_width), f32),
        cost_estimate=pl.CostEstimate(flops=1 << 30, bytes_accessed=1 << 22, transcendentals=0),
        name="synthesis",
    )(halo, coef_dual, *row_tables, *col_tables)


def analysis(extrap, halo, coef_dual):
    rows, image_width = extrap.shape
    half_rows = rows // 2
    half_width = image_width // 2
    row_tables = split_constant(row_matrix_down(rows, halo.shape[0]))
    col_tables = split_constant(col_matrix_down())

    def kernel(ext_ref, halo_ref, coef_ref, rh, rl, ch, cl, out_ref, sum_ref):
        ext = jnp.concatenate([ext_ref[...], halo_ref[...]], axis=0)
        sides = split_here(dot_three(dot_nn, (rh[...], rl[...]), split_here(ext)))
        count = half_width // LANES
        total = jnp.zeros((half_rows, LANES), f32)
        for j in range(count):
            here = slice(2 * j * LANES, 2 * (j + 1) * LANES)
            after = 2 * ((j + 1) % count)
            tail = slice(after * LANES, (after + 1) * LANES)
            operands = tuple(
                jnp.concatenate([sides[p][:, here], sides[p][:, tail]], axis=1) for p in range(2)
            )
            both = dot_three(dot_nn, operands, (ch[...], cl[...]))
            span = slice(j * LANES, (j + 1) * LANES)
            for index, part in enumerate(
                (
                    both[:half_rows, :LANES],
                    both[:half_rows, LANES:],
                    both[half_rows:, :LANES],
                    both[half_rows:, LANES:],
                )
            ):
                total = total + jnp.abs(part)
                out_ref[index, :, span] = coef_ref[index, :, span] + part
        sum_ref[...] = jnp.sum(total.reshape(half_rows // 8, 8, LANES), axis=0)

    return pl.pallas_call(
        kernel,
        out_shape=[
            jax.ShapeDtypeStruct(coef_dual.shape, f32),
            jax.ShapeDtypeStruct((8, LANES), f32),
        ],
        cost_estimate=pl.CostEstimate(flops=1 << 30, bytes_accessed=1 << 22, transcendentals=0),
        name="analysis",
    )(extrap, halo, coef_dual, *row_tables, *col_tables)


def stacked(value, axis, masks, place=0):
    return jnp.stack([value] + [flipped(value, axis, mask) for mask in masks], axis=place)


def exchanged(values):
    count = lax.axis_size(AXES)
    sent = jnp.broadcast_to(values[None, :], (count, values.shape[0]))
    return lax.all_to_all(sent, AXES, split_axis=0, concat_axis=0, tiled=True)


def local(sky_image, coef_dual, vis_dual, visibilities, kernel_blocks, tile_rows, tile_counts):
    band_count = lax.axis_size("band")
    group_count = lax.axis_size("vis")
    band_here = lax.axis_index("band")
    group_here = lax.axis_index("vis")
    device = band_here * group_count + group_here
    kernel_here = kernel_blocks[0, 0]
    rows_here = tile_rows[0, 0]
    owners, slot_count = rows_here.shape
    rows, image_width = sky_image.shape
    stripe = image_width // band_count
    samples, length = kernel_here.shape[-2:]
    half_rows = coef_dual.shape[1]
    outer = image_width // LANES
    inner = image_width // outer
    vis_tiles = owners * slot_count
    far = group_count // 4
    tiles = min(far * vis_tiles, max(vis_tiles, 256))
    blocks_f = far * vis_tiles // tiles
    masks_x = tuple(range(1, band_count))
    masks_z = tuple(range(4, group_count, 4))

    live_slots = (
        jnp.arange(slot_count, dtype=jnp.int32)[None, :] < tile_counts[0, 0][:, None]
    ).astype(f32)[:, :, None, None]
    vis_data = visibilities[0, 0]
    vis_state = vis_dual[0, 0]

    cell = band_here * stripe + rows_here.reshape(-1)
    mirrored = cell % outer > outer // 2
    kept_cell = jnp.where(mirrored, image_width - cell, cell)
    code = (kept_cell % outer) * inner + kept_cell // outer + jnp.where(mirrored, FLAG, 0)
    data_part = jnp.sum(live_slots * vis_data * vis_data)
    told = exchanged(jnp.concatenate([code.astype(f32), data_part[None]]))
    data_square = jnp.sum(told[:, vis_tiles])
    by_core = jnp.arange(2)[:, None, None, None]
    by_y = 2 * jnp.arange(2)[None, :, None, None]
    by_x = jnp.arange(band_count)[None, None, :, None]
    by_z = 4 * jnp.arange(far)[None, None, None, :]
    origin = (band_here ^ by_x) * group_count + (group_here ^ (by_core + by_y + by_z))
    chosen = origin.reshape(-1, 1) == jnp.arange(band_count * group_count)[None, :]
    codes = jnp.dot(chosen.astype(f32), told, precision=lax.Precision.HIGHEST)
    codes = jnp.round(codes[:, :vis_tiles]).astype(jnp.int32)
    codes = codes.reshape(4 * band_count * blocks_f, 1, tiles)

    lead = min(8, half_rows)
    coef_halo = shifted(coef_dual[:, half_rows - lead :, :], AXES, 1)

    weights = (live_slots * vis_state).astype(bf16)
    kernel_flat = kernel_here.reshape(vis_tiles, 2 * samples, length)
    weight_real = weights[:, :, 0].reshape(vis_tiles, samples)
    weight_imag = weights[:, :, 1].reshape(vis_tiles, samples)
    weight_pair = jnp.stack(
        [
            jnp.concatenate([weight_real, weight_imag], axis=1),
            jnp.concatenate([weight_imag, -weight_real], axis=1),
        ]
    )
    sent = jnp.einsum("nmt,ynm->ynt", kernel_flat, weight_pair, preferred_element_type=f32)
    sent = sent.astype(bf16)

    own_rows = device * rows + jnp.arange(rows, dtype=jnp.int32)

    def turns(steps):
        angle = (2.0 * math.pi / image_width) * (steps % image_width).astype(f32)
        return jnp.cos(angle), jnp.sin(angle)

    wave_cos, wave_sin = turns(own_rows[:, None] * jnp.arange(length, dtype=jnp.int32)[None, :])
    scale = 1.0 / image_width
    weight_tables = (
        *split_two(scale * jnp.concatenate([wave_cos, wave_sin], axis=0)),
        *split_two(scale * jnp.concatenate([-wave_sin, wave_cos], axis=0)),
    )
    owner_of = jnp.arange(tiles, dtype=jnp.int32) // slot_count % owners
    phases = turns(own_rows[:, None] * (owner_of * length)[None, :])
    phases_turned = tuple(p.T for p in phases)

    level = stacked(sent, "vis", masks_z, 1)
    level, weight_tables, phases, phases_turned = lax.optimization_barrier(
        (level, weight_tables, phases, phases_turned)
    )
    tile_real = stacked(level[0], "band", masks_x)
    tile_imag = stacked(level[1], "vis", (2,))
    smooth = synthesis(coef_halo, coef_dual)
    tile_real, tile_imag, smooth = lax.optimization_barrier((tile_real, tile_imag, smooth))
    tile_real = stacked(tile_real, "vis", (2,))
    tile_imag = stacked(tile_imag, "band", masks_x)
    tile_real = stacked(tile_real, "vis", (1,))
    tile_imag = stacked(tile_imag, "vis", (1,))
    tile_real = tile_real.reshape(2, 2, band_count, blocks_f, tiles, length)
    tile_imag = tile_imag.reshape(2, band_count, 2, blocks_f, tiles, length)

    new_image, extrap, spectrum = adjoint_map(
        tile_real, tile_imag, codes, weight_tables, phases, sky_image, smooth
    )

    parts = [
        forward_parts(spectrum, codes, weight_tables, phases_turned, part, (2, band_count, blocks_f))
        for part in (1, 0)
    ]
    paired = parts[1] + flipped(parts[0], "vis", 1)
    part_real = paired[0, 0] + flipped(paired[0, 1], "vis", 2)
    part_imag = paired[1, :, 0]
    for mask in masks_x:
        part_imag = part_imag + flipped(paired[1, :, mask], "band", mask)
    part_imag = part_imag[0] + flipped(part_imag[1], "vis", 2)
    left_real = part_real[0]
    for mask in masks_x:
        left_real = left_real + flipped(part_real[mask], "band", mask)
    left = jnp.stack([left_real, part_imag]).reshape(2, far, vis_tiles, length)
    seen = left[:, 0]
    for index, mask in enumerate(masks_z):
        seen = seen + flipped(left[:, 1 + index], "vis", mask)

    image_halo = shifted(extrap[: min(8, rows)], AXES, -1)
    moved_coef, abs_parts = analysis(extrap, image_halo, coef_dual)

    seen = lax.reduce_precision(seen, 8, 7).astype(bf16)
    met = jnp.einsum("nmt,ynt->nym", kernel_flat, seen, preferred_element_type=f32)
    predicted = jnp.stack(
        [
            met[:, 0, :samples] - met[:, 1, samples:],
            met[:, 1, :samples] + met[:, 0, samples:],
        ],
        axis=1,
    ).reshape(vis_state.shape)
    residual = live_slots * (vis_state + predicted - vis_data)
    sums = jnp.sum(
        exchanged(jnp.stack([jnp.sum(residual * residual), jnp.sum(abs_parts)])), axis=0
    )
    threshold = 0.5 * sums[1] / (image_width * image_width)
    new_coef = jnp.clip(moved_coef, -threshold, threshold)
    radius = 0.5 * jnp.sqrt(data_square + 1e-06)
    size_value = jnp.sqrt(sums[0] + 1e-06)
    new_vis = residual * (1.0 - jnp.minimum(1.0, radius / size_value))
    return (new_image, new_coef, new_vis[None, None])


def solution(mesh):
    return jax.shard_map(
        local,
        mesh=mesh,
        in_specs=(
            P(("band", "vis"), None),
            P(None, ("band", "vis"), None),
            P("band", "vis", None, None, None, None),
            P("band", "vis", None, None, None, None),
            P("band", "vis", None, None, None, None, None),
            P("band", "vis", None, None),
            P("band", "vis", None),
        ),
        out_specs=(
            P(("band", "vis"), None),
            P(None, ("band", "vis"), None),
            P("band", "vis", None, None, None, None),
        ),
        check_vma=False,
    )
```

```python
import math

import jax
import jax.numpy as jnp
import numpy as np
from jax import lax
from jax.experimental import pallas as pl
from jax.experimental.pallas import tpu as pltpu
from jax.sharding import PartitionSpec as P


LANES = 128
FLAG = 1 << 20

low_taps = (
    -0.010597401784997278,
    0.032883011666982945,
    0.030841381835986965,
    -0.18703481171888114,
    -0.02798376941698385,
    0.6308807679295904,
    0.7148465705525415,
    0.23037781330885523,
)
high_taps = tuple(((-1.0) ** offset * low_taps[7 - offset] for offset in range(8)))
AXES = ("band", "vis")
bf16 = jnp.bfloat16
f32 = jnp.float32


def shifted(block, axis, distance):
    devices = range(lax.axis_size(axis))
    route = [((i - distance) % len(devices), i) for i in devices]
    return lax.ppermute(block, axis, route)


def flipped(block, axis, mask):
    return lax.ppermute(block, axis, [(i, i ^ mask) for i in range(lax.axis_size(axis))])


def split_two(values):
    high = lax.reduce_precision(values, 8, 7)
    return high.astype(bf16), (values - high).astype(bf16)


def split_here(values):
    high = values.astype(bf16)
    return high, (values - high.astype(f32)).astype(bf16)


def dot_nn(left, right):
    return lax.dot_general(left, right, (((1,), (0,)), ((), ())), preferred_element_type=f32)


def dot_nt(left, right):
    return lax.dot_general(left, right, (((1,), (1,)), ((), ())), preferred_element_type=f32)


def dot_three(dot, left, right):
    return dot(left[0], right[0]) + dot(left[0], right[1]) + dot(left[1], right[0])


def scaled_sum(terms):
    total = None
    for weight, value in terms:
        if abs(weight) < 1e-12:
            continue
        part = value if weight == 1.0 else weight * value
        total = part if total is None else total + part
    return total


def cosine_sums(values, size):
    if size == 1:
        return [values[0] + values[1], values[0] - values[1]]
    half = size // 2
    even = cosine_sums(values[0::2], half)
    out = [None] * (size + 1)
    for a in range(half):
        odd = scaled_sum(
            [(math.cos(math.pi * k * a / size) if a else 1.0, values[k]) for k in range(1, size, 2)]
        )
        out[a] = even[a] + odd
        out[size - a] = even[a] - odd
    out[half] = even[half]
    return out


def sine_sums(values, size):
    half = size // 2
    out = [None] * (size + 1)
    if size == 2:
        out[1] = values[1]
        return out
    even = sine_sums(values[0::2], half)
    for a in range(1, half):
        odd = scaled_sum([(math.sin(math.pi * k * a / size), values[k]) for k in range(1, size, 2)])
        out[a] = odd + even[a]
        out[size - a] = odd - even[a]
    out[half] = scaled_sum([(math.sin(math.pi * k / 2), values[k]) for k in range(1, size, 2)])
    return out


def twiddle_seeds(image_width):
    outer = image_width // LANES
    kept = outer // 2 + 1
    inner = image_width // outer
    c = np.arange(LANES)
    one = 2.0 * np.pi * (np.arange(kept)[:, None] * c[None, :] % image_width) / image_width
    two = 2.0 * np.pi * (np.arange(inner)[:, None] * c[None, :] % inner) / inner
    one = np.stack([np.cos(one), np.sin(one)], axis=1).astype(np.float32)
    two = np.stack([np.cos(two), np.sin(two)]).astype(np.float32)
    return jnp.asarray(one), jnp.asarray(two)


def upright(row):
    return jnp.broadcast_to(row, (8, row.shape[1])).T[:, 0:1]


def sign_of(code):
    return jnp.where(code >= FLAG, -1.0, 1.0).astype(f32)


def vmem():
    return pl.BlockSpec(memory_space=pltpu.VMEM)


def emit_part(xr, xi, where, code_ref, tables, turned, real_out, imag_out, pr_ref, pi_ref):
    tiles = pr_ref.shape[0]
    together = 16
    wrh, wrl, wih, wil = tables
    pc, ps = turned

    def body(chunk, inside):
        begin = chunk * together
        spots = [where[0, begin + u] for u in range(together)]
        found = [(xr[pl.ds(at, 1), :], xi[pl.ds(at, 1), :]) for at in spots]
        for u in range(together):
            pr_ref[pl.ds(begin + u, 1), :] = found[u][0]
            pi_ref[pl.ds(begin + u, 1), :] = found[u][1]
        return inside

    lax.fori_loop(0, tiles // together, body, 0)
    sign = upright(sign_of(code_ref[...]))
    real = pr_ref[...]
    imag = pi_ref[...] * sign
    turned_re = pc[...] * real + ps[...] * imag
    turned_im = pc[...] * imag - ps[...] * real
    both = split_here(jnp.concatenate([turned_re, turned_im], axis=1))
    real_out[...] = dot_three(dot_nn, both, (wrh[...], wrl[...])).astype(real_out.dtype)
    imag_out[...] = dot_three(dot_nn, both, (wih[...], wil[...])).astype(imag_out.dtype)


def swapped(block, blocks_a, blocks_b, blocks_f):
    f, j = block % blocks_f, block // blocks_f
    return (j % blocks_b * blocks_a + j // blocks_b) * blocks_f + f


def image_step(
    tile_arrays, codes, columns, weight_tables, phases_turned, sky_image, smooth, held_as
):
    blocks_a, blocks_b, blocks_f, tiles, length = tile_arrays[0].shape
    part = blocks_a * blocks_b * blocks_f
    rows, image_width = sky_image.shape
    outer = image_width // LANES
    kept = outer // 2 + 1
    inner = image_width // outer
    width = kept * inner
    near = min(8, rows)
    seeds = twiddle_seeds(image_width)
    each = -(-kept // (2 * part))
    counts = (blocks_a, blocks_b, blocks_f)

    def kernel(
        tre, tim, tre_far, tim_far, where, code_ref, wrh, wrl, wih, wil, qc, qs,
        one, two, sky_any, smo_any,
        new_any, near_ref, xr_ref, xi_ref, real_out, imag_out,
        grid_ref, mid_ref, y_ref, mh, ml, sky, smo, new_ref, pr_ref, pi_ref, tre_in, tim_in, pc, ps, sems,
    ):
        sky_copy = pltpu.make_async_copy(sky_any, sky, sems.at[0])
        smo_copy = pltpu.make_async_copy(smo_any, smo, sems.at[1])
        tre_copy = pltpu.make_async_copy(tre_far, tre_in, sems.at[3])
        tim_copy = pltpu.make_async_copy(tim_far, tim_in, sems.at[4])
        tre_copy.start()
        tim_copy.start()
        sky_copy.start()
        smo_copy.start()
        pc[...] = qc[...].T
        ps[...] = qs[...].T
        grid_ref[...] = jnp.zeros_like(grid_ref)

        def scatter(i, carry, re_ref, im_ref, begin):
            f, j = i % blocks_f, i // blocks_f
            y, x = j // blocks_b, j % blocks_b
            re = re_ref[y, x, f]
            im = im_ref[x, y, f]
            half = (
                dot_nt(wrh[...], re) + dot_nt(wrl[...], re)
                + dot_nt(wih[...], im) + dot_nt(wil[...], im)
            )
            half_re = half[:rows]
            half_im = half[rows:]
            code = code_ref[begin + i]
            turned_re = pc[...] * half_re - ps[...] * half_im
            turned_im = (pc[...] * half_im + ps[...] * half_re) * sign_of(code)
            turned = jnp.concatenate([turned_re, turned_im], axis=0).astype(bf16)
            column = upright(code & (FLAG - 1))
            lanes = lax.broadcasted_iota(jnp.int32, (tiles, inner), 1)
            within = (lanes == column % inner).astype(f32).astype(bf16)
            major = jnp.broadcast_to((column // inner).astype(f32), (tiles, inner)).astype(bf16)
            zero = jnp.zeros_like(within)
            for first in range(0, kept, 2):
                hots = [
                    jnp.where(major == jnp.asarray(k, bf16), within, zero)
                    for k in range(first, min(first + 2, kept))
                ]
                span = slice(first * inner, (first + len(hots)) * inner)
                grid_ref[:, span] += dot_nn(turned, jnp.concatenate(hots, axis=1))
            for u in range(each):
                k = jnp.minimum((begin + i) * each + u, kept - 1)
                c1 = one[k, 0:1, :]
                s1 = one[k, 1:2, :]
                c2 = two[0]
                s2 = two[1]
                real = split_here(c1 * c2 - s1 * s2)
                imag = split_here(c1 * s2 + s1 * c2)
                for out, re, im in ((mh, real[0], imag[0]), (ml, real[1], imag[1])):
                    out[k, 0:inner, 0:LANES] = re
                    out[k, 0:inner, LANES : 2 * LANES] = im
                    out[k, inner : 2 * inner, 0:LANES] = -im
                    out[k, inner : 2 * inner, LANES : 2 * LANES] = re
            return carry

        lax.fori_loop(0, part, lambda i, c: scatter(i, c, tre, tim, 0), 0)
        tre_copy.wait()
        tim_copy.wait()
        lax.fori_loop(0, part, lambda i, c: scatter(i, c, tre_in, tim_in, part), 0)

        for k in range(kept):
            cell = jnp.concatenate(
                [
                    grid_ref[:rows, k * inner : (k + 1) * inner],
                    grid_ref[rows:, k * inner : (k + 1) * inner],
                ],
                axis=1,
            )
            mid_ref[k] = dot_three(dot_nn, split_here(cell), (mh[k], ml[k]))

        def body(chunk, carry):
            at = pl.ds(pl.multiple_of(chunk * 8, 8), 8)
            real = [mid_ref[k, at, 0:LANES] for k in range(kept)]
            imag = [mid_ref[k, at, LANES : 2 * LANES] for k in range(kept)]
            even = cosine_sums(real, outer // 2)
            odd = sine_sums(imag, outer // 2)
            values = []
            for a in range(outer):
                if a == 0 or a == outer // 2:
                    back = even[a]
                elif a < outer // 2:
                    back = even[a] - odd[a]
                else:
                    back = even[outer - a] + odd[outer - a]
                span = slice(a * LANES, (a + 1) * LANES)
                old = sky[at, span]
                new = jnp.maximum(old - smo[at, span] - back, 0.0)
                new_ref[at, span] = new
                values.append(2.0 * new - old)
            mirrored = outer // 2
            even = [values[0]]
            odd = [None]
            for a in range(1, mirrored):
                even.append(values[a] + values[outer - a])
                odd.append(values[a] - values[outer - a])
            even.append(values[mirrored])
            odd.append(None)
            real = cosine_sums(even, mirrored)
            imag = sine_sums(odd, mirrored)
            for k in range(kept):
                y_ref[k, at, 0:LANES] = real[k]
                y_ref[k, at, LANES : 2 * LANES] = (
                    jnp.zeros_like(real[k]) if imag[k] is None else -imag[k]
                )
            return carry

        sky_copy.wait()
        smo_copy.wait()
        lax.fori_loop(0, rows // 8, body, 0)
        near_ref[...] = 2.0 * new_ref[:near, :] - sky[:near, :]
        written = pltpu.make_async_copy(new_ref, new_any, sems.at[2])
        written.start()
        for k in range(kept):
            high, low = split_here(y_ref[k])
            if rows % LANES == 0:
                both = dot_nt(mh[k], jnp.concatenate([high, low], axis=0))
                both = both[:, :rows] + both[:, rows:] + dot_nt(ml[k], high)
            else:
                both = dot_three(dot_nt, (mh[k], ml[k]), (high, low))
            xr_ref[k * inner : (k + 1) * inner, :] = both[:inner]
            xi_ref[k * inner : (k + 1) * inner, :] = both[inner:]

        def emit(i, carry):
            emit_part(
                xr_ref, xi_ref, where.at[part + i], code_ref.at[part + i], (wrh, wrl, wih, wil), (qc, qs),
                real_out.at[i], imag_out.at[swapped(i, *counts)], pr_ref, pi_ref,
            )
            return carry

        lax.fori_loop(0, part, emit, 0)
        written.wait()

    any_space = pl.BlockSpec(memory_space=pl.ANY)
    return pl.pallas_call(
        kernel,
        in_specs=[
            *[vmem()] * 2,
            any_space,
            any_space,
            pl.BlockSpec(memory_space=pltpu.SMEM),
            *[vmem()] * (1 + 4 + 2 + 2),
            any_space,
            any_space,
        ],
        out_specs=[any_space] + [vmem()] * 5,
        out_shape=[
            jax.ShapeDtypeStruct((rows, image_width), f32),
            jax.ShapeDtypeStruct((near, image_width), f32),
            jax.ShapeDtypeStruct((width, rows), f32),
            jax.ShapeDtypeStruct((width, rows), f32),
            jax.ShapeDtypeStruct((part, tiles, length), held_as),
            jax.ShapeDtypeStruct((part, tiles, length), held_as),
        ],
        scratch_shapes=[
            pltpu.VMEM((2 * rows, width), f32),
            pltpu.VMEM((kept, rows, 2 * LANES), f32),
            pltpu.VMEM((kept, rows, 2 * LANES), f32),
            pltpu.VMEM((kept, 2 * inner, 2 * LANES), bf16),
            pltpu.VMEM((kept, 2 * inner, 2 * LANES), bf16),
            pltpu.VMEM((rows, image_width), f32),
            pltpu.VMEM((rows, image_width), f32),
            pltpu.VMEM((rows, image_width), f32),
            pltpu.VMEM((tiles, rows), f32),
            pltpu.VMEM((tiles, rows), f32),
            pltpu.VMEM(tile_arrays[2].shape, bf16),
            pltpu.VMEM(tile_arrays[3].shape, bf16),
            pltpu.VMEM((rows, tiles), f32),
            pltpu.VMEM((rows, tiles), f32),
            pltpu.SemaphoreType.DMA((5,)),
        ],
        cost_estimate=pl.CostEstimate(
            flops=16 * part * rows * tiles * (width + length), bytes_accessed=1 << 24, transcendentals=0
        ),
        name="image_step",
    )(
        *tile_arrays, columns, codes, *weight_tables, *phases_turned, *seeds,
        sky_image, smooth,
    )


def forward_parts(spectra, codes, columns, weight_tables, phases_turned, counts):
    tiles = codes.shape[2]
    part = math.prod(counts)
    rows = spectra[0].shape[1]
    length = weight_tables[0].shape[1]

    def kernel(
        xr, xi, where, code_ref, wrh, wrl, wih, wil, qc, qs, real_out, imag_out, pr_ref, pi_ref
    ):
        emit_part(
            xr, xi, where.at[0], code_ref.at[0], (wrh, wrl, wih, wil), (qc, qs),
            real_out.at[0], imag_out.at[0], pr_ref, pi_ref,
        )

    def whole(array):
        return pl.BlockSpec(array.shape, lambda i: (0,) * array.ndim)

    shape = jax.ShapeDtypeStruct((part, tiles, length), f32)
    return pl.pallas_call(
        kernel,
        grid=(part,),
        in_specs=[
            *[whole(x) for x in spectra],
            pl.BlockSpec((1, 1, tiles), lambda i: (i, 0, 0), memory_space=pltpu.SMEM),
            pl.BlockSpec((1, 1, tiles), lambda i: (i, 0, 0)),
            *[whole(x) for x in (*weight_tables, *phases_turned)],
        ],
        out_specs=[
            pl.BlockSpec((1, tiles, length), lambda i: (i, 0, 0)),
            pl.BlockSpec((1, tiles, length), lambda i: (swapped(i, *counts), 0, 0)),
        ],
        out_shape=[shape, shape],
        scratch_shapes=[pltpu.VMEM((tiles, rows), f32)] * 2,
        cost_estimate=pl.CostEstimate(
            flops=24 * part * rows * tiles * length, bytes_accessed=1 << 23, transcendentals=0
        ),
        name="parts",
    )(*spectra, columns, codes, *weight_tables, *phases_turned)


def row_matrix_up(half_rows, lead):
    ext = half_rows + lead
    matrix = np.zeros((2 * half_rows, 2 * ext), np.float64)
    for n in range(2 * half_rows):
        for k in range(-3, half_rows):
            tap = n - 2 * k
            if 0 <= tap < 8:
                matrix[n, lead + k] = low_taps[tap]
                matrix[n, ext + lead + k] = high_taps[tap]
    return matrix


def row_matrix_down(rows, tail):
    matrix = np.zeros((rows, rows + tail), np.float64)
    for k in range(rows // 2):
        for j in range(8):
            matrix[k, 2 * k + j] = low_taps[j]
            matrix[rows // 2 + k, 2 * k + j] = high_taps[j]
    return matrix


def col_matrix_up():
    matrix = np.zeros((4, LANES, 2 * LANES), np.float64)
    for n in range(2 * LANES):
        for k in range(-LANES, LANES):
            tap = n - 2 * k
            if 0 <= tap < 8:
                where = (0, k + LANES) if k < 0 else (1, k)
                matrix[where[0], where[1], n] = low_taps[tap]
                matrix[2 + where[0], where[1], n] = high_taps[tap]
    return matrix.reshape(4 * LANES, 2 * LANES)


def col_matrix_down():
    matrix = np.zeros((3 * LANES, 2 * LANES), np.float64)
    for k in range(LANES):
        for j in range(8):
            matrix[2 * k + j, k] = low_taps[j]
            matrix[2 * k + j, LANES + k] = high_taps[j]
    return matrix


def split_constant(matrix):
    value = np.asarray(matrix, np.float32)
    high = value.astype(bf16)
    low = (value - high.astype(np.float32)).astype(bf16)
    return jnp.asarray(high), jnp.asarray(low)


def synthesis(halo, coef_dual):
    _, half_rows, half_width = coef_dual.shape
    rows = 2 * half_rows
    lead = halo.shape[1]
    row_tables = split_constant(row_matrix_up(half_rows, lead))
    col_tables = split_constant(col_matrix_up())

    def kernel(halo_ref, coef_ref, rh, rl, ch, cl, out_ref):
        sides = []
        for first, second in ((0, 2), (1, 3)):
            ext = jnp.concatenate(
                [halo_ref[first], coef_ref[first], halo_ref[second], coef_ref[second]], axis=0
            )
            sides.append(dot_three(dot_nn, (rh[...], rl[...]), split_here(ext)))
        low = split_here(sides[0])
        high = split_here(sides[1])
        count = half_width // LANES
        for j in range(count):
            here = slice(j * LANES, (j + 1) * LANES)
            past = (j - 1) % count
            before = slice(past * LANES, (past + 1) * LANES)
            operands = tuple(
                jnp.concatenate(
                    [low[p][:, before], low[p][:, here], high[p][:, before], high[p][:, here]],
                    axis=1,
                )
                for p in range(2)
            )
            out_ref[:, 2 * j * LANES : 2 * (j + 1) * LANES] = dot_three(
                dot_nn, operands, (ch[...], cl[...])
            )

    return pl.pallas_call(
        kernel,
        out_shape=jax.ShapeDtypeStruct((rows, 2 * half_width), f32),
        cost_estimate=pl.CostEstimate(flops=1 << 30, bytes_accessed=1 << 22, transcendentals=0),
        name="synthesis",
    )(halo, coef_dual, *row_tables, *col_tables)


def analysis(new_image, sky_image, halo, coef_dual):
    rows, image_width = new_image.shape
    half_rows = rows // 2
    half_width = image_width // 2
    row_tables = split_constant(row_matrix_down(rows, halo.shape[0]))
    col_tables = split_constant(col_matrix_down())

    def kernel(new_ref, sky_ref, halo_ref, coef_ref, rh, rl, ch, cl, out_ref, sum_ref):
        extrap = 2.0 * new_ref[...] - sky_ref[...]
        ext = jnp.concatenate([extrap, halo_ref[...]], axis=0)
        sides = split_here(dot_three(dot_nn, (rh[...], rl[...]), split_here(ext)))
        count = half_width // LANES
        total = jnp.zeros((half_rows, LANES), f32)
        for j in range(count):
            here = slice(2 * j * LANES, 2 * (j + 1) * LANES)
            after = 2 * ((j + 1) % count)
            tail = slice(after * LANES, (after + 1) * LANES)
            operands = tuple(
                jnp.concatenate([sides[p][:, here], sides[p][:, tail]], axis=1) for p in range(2)
            )
            both = dot_three(dot_nn, operands, (ch[...], cl[...]))
            span = slice(j * LANES, (j + 1) * LANES)
            for index, part in enumerate(
                (
                    both[:half_rows, :LANES],
                    both[:half_rows, LANES:],
                    both[half_rows:, :LANES],
                    both[half_rows:, LANES:],
                )
            ):
                total = total + jnp.abs(part)
                out_ref[index, :, span] = coef_ref[index, :, span] + part
        sum_ref[...] = jnp.sum(total, axis=0, keepdims=True)

    return pl.pallas_call(
        kernel,
        out_shape=[
            jax.ShapeDtypeStruct(coef_dual.shape, f32),
            jax.ShapeDtypeStruct((1, LANES), f32),
        ],
        cost_estimate=pl.CostEstimate(flops=1 << 30, bytes_accessed=1 << 22, transcendentals=0),
        name="analysis",
    )(new_image, sky_image, halo, coef_dual, *row_tables, *col_tables)


def joined(value, axis, masks, place=0):
    return jnp.concatenate([value] + [flipped(value, axis, mask) for mask in masks], axis=place)


def exchanged(values):
    count = lax.axis_size(AXES)
    sent = jnp.broadcast_to(values[None, :], (count, values.shape[0]))
    return lax.all_to_all(sent, AXES, split_axis=0, concat_axis=0, tiled=True)


def local(sky_image, coef_dual, vis_dual, visibilities, kernel_blocks, tile_rows, tile_counts):
    band_count = lax.axis_size("band")
    group_count = lax.axis_size("vis")
    band_here = lax.axis_index("band")
    group_here = lax.axis_index("vis")
    device = band_here * group_count + group_here
    kernel_here = kernel_blocks[0, 0]
    rows_here = tile_rows[0, 0]
    owners, slot_count = rows_here.shape
    rows, image_width = sky_image.shape
    stripe = image_width // band_count
    samples, length = kernel_here.shape[-2:]
    half_rows = coef_dual.shape[1]
    outer = image_width // LANES
    inner = image_width // outer
    vis_tiles = owners * slot_count
    far = group_count // 4
    tiles = min(far * vis_tiles, max(vis_tiles, 256))
    blocks_f = far * vis_tiles // tiles
    masks_x = tuple(range(1, band_count))
    masks_z = tuple(range(4, group_count, 4))

    live_slots = (
        jnp.arange(slot_count, dtype=jnp.int32)[None, :] < tile_counts[0, 0][:, None]
    ).astype(f32)[:, :, None, None]
    vis_data = visibilities[0, 0]
    vis_state = vis_dual[0, 0]

    cell = band_here * stripe + rows_here.reshape(-1)
    mirrored = cell % outer > outer // 2
    kept_cell = jnp.where(mirrored, image_width - cell, cell)
    code = (kept_cell % outer) * inner + kept_cell // outer + jnp.where(mirrored, FLAG, 0)
    told = exchanged(code.astype(f32))
    by_core = jnp.arange(2)[:, None, None, None]
    by_y = 2 * jnp.arange(2)[None, :, None, None]
    by_x = jnp.arange(band_count)[None, None, :, None]
    by_z = 4 * jnp.arange(far)[None, None, None, :]
    origin = (band_here ^ by_x) * group_count + (group_here ^ (by_core + by_y + by_z))
    chosen = origin.reshape(-1, 1) == jnp.arange(band_count * group_count)[None, :]
    codes = jnp.dot(chosen.astype(f32), told, precision=lax.Precision.HIGHEST)
    codes = jnp.round(codes).astype(jnp.int32)
    codes = codes.reshape(4 * band_count * blocks_f, 1, tiles)
    columns = codes & (FLAG - 1)

    lead = min(8, half_rows)
    coef_halo = shifted(coef_dual[:, half_rows - lead :, :], AXES, 1)

    weights = (live_slots * vis_state).astype(bf16)
    kernel_flat = kernel_here.reshape(vis_tiles, 2 * samples, length)
    weight_real = weights[:, :, 0].reshape(vis_tiles, samples)
    weight_imag = weights[:, :, 1].reshape(vis_tiles, samples)
    weight_pair = jnp.stack(
        [
            jnp.concatenate([weight_real, weight_imag], axis=1),
            jnp.concatenate([weight_imag, -weight_real], axis=1),
        ]
    )
    sent = jnp.einsum("nmt,ynm->ynt", kernel_flat, weight_pair, preferred_element_type=f32)
    sent = sent.astype(bf16)

    def unit(steps):
        angle = (2.0 * math.pi / image_width) * (steps % image_width).astype(f32)
        return jnp.cos(angle), jnp.sin(angle)

    def turned_by(steps, axis):
        near = np.arange(rows)[:, None] * steps[None, :] % image_width * (2.0 * np.pi / image_width)
        near = near if axis else near.T
        near_cos = np.cos(near).astype(np.float32)
        near_sin = np.sin(near).astype(np.float32)
        far_cos, far_sin = unit(device * rows * jnp.expand_dims(jnp.asarray(steps, jnp.int32), 1 - axis))
        return (
            near_cos * far_cos - near_sin * far_sin,
            near_sin * far_cos + near_cos * far_sin,
        )

    wave_cos, wave_sin = turned_by(np.arange(length), 1)
    scale = 1.0 / image_width
    weight_tables = (
        *split_two(scale * jnp.concatenate([wave_cos, wave_sin], axis=0)),
        *split_two(scale * jnp.concatenate([-wave_sin, wave_cos], axis=0)),
    )
    phases_turned = turned_by(np.arange(tiles) // slot_count % owners * length, 0)
    data_parts = jnp.sum(live_slots * vis_data * vis_data, axis=(0, 1)).reshape(-1)
    phases_turned, data_parts = lax.optimization_barrier((phases_turned, data_parts))

    level = joined(sent, "vis", masks_z, 1)
    tile_real = joined(level[0], "band", masks_x)
    tile_imag = joined(level[1], "vis", (2,))
    tile_real = joined(tile_real, "vis", (2,))
    tile_imag = joined(tile_imag, "band", masks_x)
    tile_real = tile_real.reshape(2, band_count, blocks_f, tiles, length)
    tile_imag = tile_imag.reshape(band_count, 2, blocks_f, tiles, length)
    far_real = flipped(tile_real, "vis", 1)
    far_imag = flipped(tile_imag, "vis", 1)
    smooth = synthesis(coef_halo, coef_dual)

    counts = (2, band_count, blocks_f)
    large = 8 * band_count * far * vis_tiles * length * 4 > 1 << 23
    new_image, near_rows, spec_real, spec_imag, sent_real, sent_imag = image_step(
        (tile_real, tile_imag, far_real, far_imag), codes, columns, weight_tables,
        phases_turned, sky_image, smooth, bf16 if large else f32,
    )
    image_halo = shifted(near_rows, AXES, -1)
    mine_real, mine_imag = forward_parts(
        (spec_real, spec_imag), codes, columns, weight_tables, phases_turned, counts
    )
    other_real = flipped(sent_real, "vis", 1)
    other_imag = flipped(sent_imag, "vis", 1)
    step_y = band_count * blocks_f
    step_x = 2 * blocks_f

    def real_at(begin, size):
        return mine_real[begin : begin + size] + other_real[begin : begin + size]

    def imag_at(begin, size):
        return mine_imag[begin : begin + size] + other_imag[begin : begin + size]

    met_real = flipped(real_at(step_y, step_y), "vis", 2)
    met_imag = [flipped(imag_at(m * step_x, step_x), "band", m) for m in masks_x]

    def real_kept(m):
        return real_at(m * blocks_f, blocks_f) + met_real[m * blocks_f : (m + 1) * blocks_f]

    def imag_kept(y):
        span = slice(y * blocks_f, (y + 1) * blocks_f)
        return sum([met[span] for met in met_imag], imag_at(y * blocks_f, blocks_f))

    left_real = [flipped(real_kept(m), "band", m) for m in masks_x]
    left_imag = flipped(imag_kept(1), "vis", 2)
    left_real = sum(left_real, real_kept(0))
    left_imag = left_imag + imag_kept(0)
    left = jnp.stack([left_real, left_imag]).reshape(2, far, vis_tiles, length)
    seen = [flipped(left[:, 1 + index], "vis", mask) for index, mask in enumerate(masks_z)]
    seen = sum(seen, left[:, 0])

    moved_coef, abs_parts = analysis(new_image, sky_image, image_halo, coef_dual)
    totals = exchanged(jnp.concatenate([abs_parts[0], data_parts]))
    coef_total = jnp.sum(totals[:, :LANES])
    data_square = jnp.sum(totals[:, LANES:])
    threshold = 0.5 * coef_total / (image_width * image_width)
    new_coef = jnp.clip(moved_coef, -threshold, threshold)

    seen = lax.reduce_precision(seen, 8, 7).astype(bf16)
    met = jnp.einsum("nmt,ynt->nym", kernel_flat, seen, preferred_element_type=f32)
    predicted = jnp.stack(
        [
            met[:, 0, :samples] - met[:, 1, samples:],
            met[:, 1, :samples] + met[:, 0, samples:],
        ],
        axis=1,
    ).reshape(vis_state.shape)
    residual = live_slots * (vis_state + predicted - vis_data)
    squares = jnp.sum(residual * residual, axis=(0, 1)).reshape(-1)
    norm_square = jnp.sum(exchanged(squares))
    radius = 0.5 * jnp.sqrt(data_square + 1e-06)
    size_value = jnp.sqrt(norm_square + 1e-06)
    new_vis = residual * (1.0 - jnp.minimum(1.0, radius / size_value))
    return (new_image, new_coef, new_vis[None, None])


def solution(mesh):
    return jax.shard_map(
        local,
        mesh=mesh,
        in_specs=(
            P(("band", "vis"), None),
            P(None, ("band", "vis"), None),
            P("band", "vis", None, None, None, None),
            P("band", "vis", None, None, None, None),
            P("band", "vis", None, None, None, None, None),
            P("band", "vis", None, None),
            P("band", "vis", None),
        ),
        out_specs=(
            P(("band", "vis"), None),
            P(None, ("band", "vis"), None),
            P("band", "vis", None, None, None, None),
        ),
        check_vma=False,
    )
```

```python
import math

import jax
import jax.numpy as jnp
import numpy as np
from jax import lax
from jax.experimental import pallas as pl
from jax.experimental.pallas import tpu as pltpu
from jax.sharding import PartitionSpec as P


LANES = 128
FLAG = 1 << 20

low_taps = (
    -0.010597401784997278,
    0.032883011666982945,
    0.030841381835986965,
    -0.18703481171888114,
    -0.02798376941698385,
    0.6308807679295904,
    0.7148465705525415,
    0.23037781330885523,
)
high_taps = tuple(((-1.0) ** offset * low_taps[7 - offset] for offset in range(8)))
AXES = ("band", "vis")
bf16 = jnp.bfloat16
f32 = jnp.float32


def shifted(block, axis, distance):
    devices = range(lax.axis_size(axis))
    route = [((i - distance) % len(devices), i) for i in devices]
    return lax.ppermute(block, axis, route)


def flipped(block, axis, mask):
    return lax.ppermute(block, axis, [(i, i ^ mask) for i in range(lax.axis_size(axis))])


def split_two(values):
    high = lax.reduce_precision(values, 8, 7)
    return high.astype(bf16), (values - high).astype(bf16)


def split_here(values):
    high = values.astype(bf16)
    return high, (values - high.astype(f32)).astype(bf16)


def dot_nn(left, right):
    return lax.dot_general(left, right, (((1,), (0,)), ((), ())), preferred_element_type=f32)


def dot_nt(left, right):
    return lax.dot_general(left, right, (((1,), (1,)), ((), ())), preferred_element_type=f32)


def dot_three(dot, left, right):
    return dot(left[0], right[0]) + dot(left[0], right[1]) + dot(left[1], right[0])


def scaled_sum(terms):
    total = None
    for weight, value in terms:
        if abs(weight) < 1e-12:
            continue
        part = value if weight == 1.0 else weight * value
        total = part if total is None else total + part
    return total


def cosine_sums(values, size):
    if size == 1:
        return [values[0] + values[1], values[0] - values[1]]
    half = size // 2
    even = cosine_sums(values[0::2], half)
    out = [None] * (size + 1)
    for a in range(half):
        odd = scaled_sum(
            [(math.cos(math.pi * k * a / size) if a else 1.0, values[k]) for k in range(1, size, 2)]
        )
        out[a] = even[a] + odd
        out[size - a] = even[a] - odd
    out[half] = even[half]
    return out


def sine_sums(values, size):
    half = size // 2
    out = [None] * (size + 1)
    if size == 2:
        out[1] = values[1]
        return out
    even = sine_sums(values[0::2], half)
    for a in range(1, half):
        odd = scaled_sum([(math.sin(math.pi * k * a / size), values[k]) for k in range(1, size, 2)])
        out[a] = odd + even[a]
        out[size - a] = odd - even[a]
    out[half] = scaled_sum([(math.sin(math.pi * k / 2), values[k]) for k in range(1, size, 2)])
    return out


def twiddle_seeds(image_width):
    outer = image_width // LANES
    kept = outer // 2 + 1
    inner = image_width // outer
    c = np.arange(LANES)
    one = 2.0 * np.pi * (np.arange(kept)[:, None] * c[None, :] % image_width) / image_width
    two = 2.0 * np.pi * (np.arange(inner)[:, None] * c[None, :] % inner) / inner
    one = np.stack([np.cos(one), np.sin(one)], axis=1).astype(np.float32)
    two = np.stack([np.cos(two), np.sin(two)]).astype(np.float32)
    return jnp.asarray(one), jnp.asarray(two)


def upright(row):
    return jnp.broadcast_to(row, (8, row.shape[1])).T[:, 0:1]


def sign_of(code):
    return jnp.where(code >= FLAG, -1.0, 1.0).astype(f32)


def vmem():
    return pl.BlockSpec(memory_space=pltpu.VMEM)


def emit_part(xr, xi, where, code_ref, tables, turned, real_out, imag_out, pr_ref, pi_ref):
    tiles = pr_ref.shape[0]
    together = 16
    wrh, wrl, wih, wil = tables
    pc, ps = turned

    def body(chunk, inside):
        begin = chunk * together
        spots = [where[0, begin + u] for u in range(together)]
        found = [(xr[pl.ds(at, 1), :], xi[pl.ds(at, 1), :]) for at in spots]
        for u in range(together):
            pr_ref[pl.ds(begin + u, 1), :] = found[u][0]
            pi_ref[pl.ds(begin + u, 1), :] = found[u][1]
        return inside

    lax.fori_loop(0, tiles // together, body, 0)
    sign = upright(sign_of(code_ref[...]))
    real = pr_ref[...]
    imag = pi_ref[...] * sign
    turned_re = pc[...] * real + ps[...] * imag
    turned_im = pc[...] * imag - ps[...] * real
    both = split_here(jnp.concatenate([turned_re, turned_im], axis=1))
    real_out[...] = dot_three(dot_nn, both, (wrh[...], wrl[...])).astype(real_out.dtype)
    imag_out[...] = dot_three(dot_nn, both, (wih[...], wil[...])).astype(imag_out.dtype)


def swapped(block, blocks_a, blocks_b, blocks_f):
    f, j = block % blocks_f, block // blocks_f
    return (j % blocks_b * blocks_a + j // blocks_b) * blocks_f + f


def image_step(
    tile_arrays, codes, columns, weight_tables, phases_turned, sky_image, smooth, held_as
):
    blocks_a, blocks_b, blocks_f, tiles, length = tile_arrays[0].shape
    part = blocks_a * blocks_b * blocks_f
    rows, image_width = sky_image.shape
    outer = image_width // LANES
    kept = outer // 2 + 1
    inner = image_width // outer
    width = kept * inner
    near = min(8, rows)
    seeds = twiddle_seeds(image_width)
    each = -(-kept // (2 * part))
    counts = (blocks_a, blocks_b, blocks_f)

    def kernel(
        tre, tim, tre_far, tim_far, where, code_ref, wrh, wrl, wih, wil, qc, qs,
        one, two, sky_any, smo_any,
        new_any, near_ref, xr_any, xi_any, real_any, imag_any,
        grid_ref, mid_ref, y_ref, mh, ml, sky, smo, new_ref, pr_ref, pi_ref, tre_in, tim_in, pc, ps,
        xr_ref, xi_ref, real_out, imag_out, sems, real_sems, imag_sems,
    ):
        sky_copy = pltpu.make_async_copy(sky_any, sky, sems.at[0])
        smo_copy = pltpu.make_async_copy(smo_any, smo, sems.at[1])
        tre_copy = pltpu.make_async_copy(tre_far, tre_in, sems.at[3])
        tim_copy = pltpu.make_async_copy(tim_far, tim_in, sems.at[4])
        tre_copy.start()
        tim_copy.start()
        sky_copy.start()
        smo_copy.start()
        pc[...] = qc[...].T
        ps[...] = qs[...].T
        grid_ref[...] = jnp.zeros_like(grid_ref)

        def scatter(i, carry, re_ref, im_ref, begin):
            f, j = i % blocks_f, i // blocks_f
            y, x = j // blocks_b, j % blocks_b
            re = re_ref[y, x, f]
            im = im_ref[x, y, f]
            half = (
                dot_nt(wrh[...], re) + dot_nt(wih[...], im)
            )
            half_re = half[:rows]
            half_im = half[rows:]
            code = code_ref[begin + i]
            turned_re = pc[...] * half_re - ps[...] * half_im
            turned_im = (pc[...] * half_im + ps[...] * half_re) * sign_of(code)
            turned = jnp.concatenate([turned_re, turned_im], axis=0).astype(bf16)
            column = upright(code & (FLAG - 1))
            lanes = lax.broadcasted_iota(jnp.int32, (tiles, inner), 1)
            within = (lanes == column % inner).astype(f32).astype(bf16)
            major = jnp.broadcast_to((column // inner).astype(f32), (tiles, inner)).astype(bf16)
            zero = jnp.zeros_like(within)
            for first in range(0, kept, 2):
                hots = [
                    jnp.where(major == jnp.asarray(k, bf16), within, zero)
                    for k in range(first, min(first + 2, kept))
                ]
                span = slice(first * inner, (first + len(hots)) * inner)
                grid_ref[:, span] += dot_nn(turned, jnp.concatenate(hots, axis=1))
            for u in range(each):
                k = jnp.minimum((begin + i) * each + u, kept - 1)
                c1 = one[k, 0:1, :]
                s1 = one[k, 1:2, :]
                c2 = two[0]
                s2 = two[1]
                real = split_here(c1 * c2 - s1 * s2)
                imag = split_here(c1 * s2 + s1 * c2)
                for out, re, im in ((mh, real[0], imag[0]), (ml, real[1], imag[1])):
                    out[k, 0:inner, 0:LANES] = re
                    out[k, 0:inner, LANES : 2 * LANES] = im
                    out[k, inner : 2 * inner, 0:LANES] = -im
                    out[k, inner : 2 * inner, LANES : 2 * LANES] = re
            return carry

        lax.fori_loop(0, part, lambda i, c: scatter(i, c, tre, tim, 0), 0)
        tre_copy.wait()
        tim_copy.wait()
        lax.fori_loop(0, part, lambda i, c: scatter(i, c, tre_in, tim_in, part), 0)

        for k in range(kept):
            cell = jnp.concatenate(
                [
                    grid_ref[:rows, k * inner : (k + 1) * inner],
                    grid_ref[rows:, k * inner : (k + 1) * inner],
                ],
                axis=1,
            )
            mid_ref[k] = dot_three(dot_nn, split_here(cell), (mh[k], ml[k]))

        def body(chunk, carry):
            at = pl.ds(pl.multiple_of(chunk * 8, 8), 8)
            real = [mid_ref[k, at, 0:LANES] for k in range(kept)]
            imag = [mid_ref[k, at, LANES : 2 * LANES] for k in range(kept)]
            even = cosine_sums(real, outer // 2)
            odd = sine_sums(imag, outer // 2)
            values = []
            for a in range(outer):
                if a == 0 or a == outer // 2:
                    back = even[a]
                elif a < outer // 2:
                    back = even[a] - odd[a]
                else:
                    back = even[outer - a] + odd[outer - a]
                span = slice(a * LANES, (a + 1) * LANES)
                old = sky[at, span]
                new = jnp.maximum(old - smo[at, span] - back, 0.0)
                new_ref[at, span] = new
                values.append(2.0 * new - old)
            mirrored = outer // 2
            even = [values[0]]
            odd = [None]
            for a in range(1, mirrored):
                even.append(values[a] + values[outer - a])
                odd.append(values[a] - values[outer - a])
            even.append(values[mirrored])
            odd.append(None)
            real = cosine_sums(even, mirrored)
            imag = sine_sums(odd, mirrored)
            for k in range(kept):
                y_ref[k, at, 0:LANES] = real[k]
                y_ref[k, at, LANES : 2 * LANES] = (
                    jnp.zeros_like(real[k]) if imag[k] is None else -imag[k]
                )
            return carry

        sky_copy.wait()
        smo_copy.wait()
        lax.fori_loop(0, rows // 8, body, 0)
        near_ref[...] = 2.0 * new_ref[:near, :] - sky[:near, :]
        written = pltpu.make_async_copy(new_ref, new_any, sems.at[2])
        written.start()
        for k in range(kept):
            high, low = split_here(y_ref[k])
            if rows % LANES == 0:
                both = dot_nt(mh[k], jnp.concatenate([high, low], axis=0))
                both = both[:, :rows] + both[:, rows:] + dot_nt(ml[k], high)
            else:
                both = dot_three(dot_nt, (mh[k], ml[k]), (high, low))
            xr_ref[k * inner : (k + 1) * inner, :] = both[:inner]
            xi_ref[k * inner : (k + 1) * inner, :] = both[inner:]

        xr_copy = pltpu.make_async_copy(xr_ref, xr_any, sems.at[5])
        xi_copy = pltpu.make_async_copy(xi_ref, xi_any, sems.at[6])
        xr_copy.start()
        xi_copy.start()

        def part_copies(i):
            j = swapped(i, *counts)
            return (
                pltpu.make_async_copy(real_out.at[i], real_any.at[i], real_sems.at[i]),
                pltpu.make_async_copy(imag_out.at[j], imag_any.at[j], imag_sems.at[i]),
            )

        def emit(i, carry):
            emit_part(
                xr_ref, xi_ref, where.at[part + i], code_ref.at[part + i], (wrh, wrl, wih, wil), (qc, qs),
                real_out.at[i], imag_out.at[swapped(i, *counts)], pr_ref, pi_ref,
            )
            for copy in part_copies(i):
                copy.start()
            return carry

        def settle(i, carry):
            for copy in part_copies(i):
                copy.wait()
            return carry

        lax.fori_loop(0, part, emit, 0)
        lax.fori_loop(0, part, settle, 0)
        xr_copy.wait()
        xi_copy.wait()
        written.wait()

    any_space = pl.BlockSpec(memory_space=pl.ANY)
    return pl.pallas_call(
        kernel,
        in_specs=[
            *[vmem()] * 2,
            any_space,
            any_space,
            pl.BlockSpec(memory_space=pltpu.SMEM),
            *[vmem()] * (1 + 4 + 2 + 2),
            any_space,
            any_space,
        ],
        out_specs=[any_space, vmem()] + [any_space] * 4,
        out_shape=[
            jax.ShapeDtypeStruct((rows, image_width), f32),
            jax.ShapeDtypeStruct((near, image_width), f32),
            jax.ShapeDtypeStruct((width, rows), f32),
            jax.ShapeDtypeStruct((width, rows), f32),
            jax.ShapeDtypeStruct((part, tiles, length), held_as),
            jax.ShapeDtypeStruct((part, tiles, length), held_as),
        ],
        scratch_shapes=[
            pltpu.VMEM((2 * rows, width), f32),
            pltpu.VMEM((kept, rows, 2 * LANES), f32),
            pltpu.VMEM((kept, rows, 2 * LANES), f32),
            pltpu.VMEM((kept, 2 * inner, 2 * LANES), bf16),
            pltpu.VMEM((kept, 2 * inner, 2 * LANES), bf16),
            pltpu.VMEM((rows, image_width), f32),
            pltpu.VMEM((rows, image_width), f32),
            pltpu.VMEM((rows, image_width), f32),
            pltpu.VMEM((tiles, rows), f32),
            pltpu.VMEM((tiles, rows), f32),
            pltpu.VMEM(tile_arrays[2].shape, bf16),
            pltpu.VMEM(tile_arrays[3].shape, bf16),
            pltpu.VMEM((rows, tiles), f32),
            pltpu.VMEM((rows, tiles), f32),
            pltpu.VMEM((width, rows), f32),
            pltpu.VMEM((width, rows), f32),
            pltpu.VMEM((part, tiles, length), held_as),
            pltpu.VMEM((part, tiles, length), held_as),
            pltpu.SemaphoreType.DMA((7,)),
            pltpu.SemaphoreType.DMA((part,)),
            pltpu.SemaphoreType.DMA((part,)),
        ],
        cost_estimate=pl.CostEstimate(
            flops=16 * part * rows * tiles * (width + length), bytes_accessed=1 << 24, transcendentals=0
        ),
        name="image_step",
    )(
        *tile_arrays, columns, codes, *weight_tables, *phases_turned, *seeds,
        sky_image, smooth,
    )


def forward_parts(spectra, codes, columns, weight_tables, phases_turned, counts):
    tiles = codes.shape[2]
    part = math.prod(counts)
    rows = spectra[0].shape[1]
    length = weight_tables[0].shape[1]

    def kernel(
        xr, xi, where, code_ref, wrh, wrl, wih, wil, qc, qs, real_out, imag_out, pr_ref, pi_ref
    ):
        emit_part(
            xr, xi, where.at[0], code_ref.at[0], (wrh, wrl, wih, wil), (qc, qs),
            real_out.at[0], imag_out.at[0], pr_ref, pi_ref,
        )

    def whole(array):
        return pl.BlockSpec(array.shape, lambda i: (0,) * array.ndim)

    shape = jax.ShapeDtypeStruct((part, tiles, length), f32)
    return pl.pallas_call(
        kernel,
        grid=(part,),
        in_specs=[
            *[whole(x) for x in spectra],
            pl.BlockSpec((1, 1, tiles), lambda i: (i, 0, 0), memory_space=pltpu.SMEM),
            pl.BlockSpec((1, 1, tiles), lambda i: (i, 0, 0)),
            *[whole(x) for x in (*weight_tables, *phases_turned)],
        ],
        out_specs=[
            pl.BlockSpec((1, tiles, length), lambda i: (i, 0, 0)),
            pl.BlockSpec((1, tiles, length), lambda i: (swapped(i, *counts), 0, 0)),
        ],
        out_shape=[shape, shape],
        scratch_shapes=[pltpu.VMEM((tiles, rows), f32)] * 2,
        cost_estimate=pl.CostEstimate(
            flops=24 * part * rows * tiles * length, bytes_accessed=1 << 23, transcendentals=0
        ),
        name="parts",
    )(*spectra, columns, codes, *weight_tables, *phases_turned)


def row_matrix_up(half_rows, lead):
    ext = half_rows + lead
    matrix = np.zeros((2 * half_rows, 2 * ext), np.float64)
    for n in range(2 * half_rows):
        for k in range(-3, half_rows):
            tap = n - 2 * k
            if 0 <= tap < 8:
                matrix[n, lead + k] = low_taps[tap]
                matrix[n, ext + lead + k] = high_taps[tap]
    return matrix


def row_matrix_down(rows, tail):
    matrix = np.zeros((rows, rows + tail), np.float64)
    for k in range(rows // 2):
        for j in range(8):
            matrix[k, 2 * k + j] = low_taps[j]
            matrix[rows // 2 + k, 2 * k + j] = high_taps[j]
    return matrix


def col_matrix_up():
    matrix = np.zeros((4, LANES, 2 * LANES), np.float64)
    for n in range(2 * LANES):
        for k in range(-LANES, LANES):
            tap = n - 2 * k
            if 0 <= tap < 8:
                where = (0, k + LANES) if k < 0 else (1, k)
                matrix[where[0], where[1], n] = low_taps[tap]
                matrix[2 + where[0], where[1], n] = high_taps[tap]
    return matrix.reshape(4 * LANES, 2 * LANES)


def col_matrix_down():
    matrix = np.zeros((3 * LANES, 2 * LANES), np.float64)
    for k in range(LANES):
        for j in range(8):
            matrix[2 * k + j, k] = low_taps[j]
            matrix[2 * k + j, LANES + k] = high_taps[j]
    return matrix


def split_constant(matrix):
    value = np.asarray(matrix, np.float32)
    high = value.astype(bf16)
    low = (value - high.astype(np.float32)).astype(bf16)
    return jnp.asarray(high), jnp.asarray(low)


def synthesis(halo, coef_dual):
    _, half_rows, half_width = coef_dual.shape
    rows = 2 * half_rows
    lead = halo.shape[1]
    row_tables = split_constant(row_matrix_up(half_rows, lead))
    col_tables = split_constant(col_matrix_up())

    def kernel(halo_ref, coef_ref, rh, rl, ch, cl, out_ref):
        sides = []
        for first, second in ((0, 2), (1, 3)):
            ext = jnp.concatenate(
                [halo_ref[first], coef_ref[first], halo_ref[second], coef_ref[second]], axis=0
            )
            sides.append(dot_three(dot_nn, (rh[...], rl[...]), split_here(ext)))
        low = split_here(sides[0])
        high = split_here(sides[1])
        count = half_width // LANES
        for j in range(count):
            here = slice(j * LANES, (j + 1) * LANES)
            past = (j - 1) % count
            before = slice(past * LANES, (past + 1) * LANES)
            operands = tuple(
                jnp.concatenate(
                    [low[p][:, before], low[p][:, here], high[p][:, before], high[p][:, here]],
                    axis=1,
                )
                for p in range(2)
            )
            out_ref[:, 2 * j * LANES : 2 * (j + 1) * LANES] = dot_three(
                dot_nn, operands, (ch[...], cl[...])
            )

    return pl.pallas_call(
        kernel,
        out_shape=jax.ShapeDtypeStruct((rows, 2 * half_width), f32),
        cost_estimate=pl.CostEstimate(flops=1 << 30, bytes_accessed=1 << 22, transcendentals=0),
        name="synthesis",
    )(halo, coef_dual, *row_tables, *col_tables)


def analysis(new_image, sky_image, halo, coef_dual):
    rows, image_width = new_image.shape
    half_rows = rows // 2
    half_width = image_width // 2
    row_tables = split_constant(row_matrix_down(rows, halo.shape[0]))
    col_tables = split_constant(col_matrix_down())

    def kernel(new_ref, sky_ref, halo_ref, coef_ref, rh, rl, ch, cl, out_ref, sum_ref):
        extrap = 2.0 * new_ref[...] - sky_ref[...]
        ext = jnp.concatenate([extrap, halo_ref[...]], axis=0)
        sides = split_here(dot_three(dot_nn, (rh[...], rl[...]), split_here(ext)))
        count = half_width // LANES
        total = jnp.zeros((half_rows, LANES), f32)
        for j in range(count):
            here = slice(2 * j * LANES, 2 * (j + 1) * LANES)
            after = 2 * ((j + 1) % count)
            tail = slice(after * LANES, (after + 1) * LANES)
            operands = tuple(
                jnp.concatenate([sides[p][:, here], sides[p][:, tail]], axis=1) for p in range(2)
            )
            both = dot_three(dot_nn, operands, (ch[...], cl[...]))
            span = slice(j * LANES, (j + 1) * LANES)
            for index, part in enumerate(
                (
                    both[:half_rows, :LANES],
                    both[:half_rows, LANES:],
                    both[half_rows:, :LANES],
                    both[half_rows:, LANES:],
                )
            ):
                total = total + jnp.abs(part)
                out_ref[index, :, span] = coef_ref[index, :, span] + part
        sum_ref[...] = jnp.sum(total, axis=0, keepdims=True)

    return pl.pallas_call(
        kernel,
        out_shape=[
            jax.ShapeDtypeStruct(coef_dual.shape, f32),
            jax.ShapeDtypeStruct((1, LANES), f32),
        ],
        cost_estimate=pl.CostEstimate(flops=1 << 30, bytes_accessed=1 << 22, transcendentals=0),
        name="analysis",
    )(new_image, sky_image, halo, coef_dual, *row_tables, *col_tables)


def joined(value, axis, masks, place=0):
    return jnp.concatenate([value] + [flipped(value, axis, mask) for mask in masks], axis=place)


def exchanged(values):
    count = lax.axis_size(AXES)
    sent = jnp.broadcast_to(values[None, :], (count, values.shape[0]))
    return lax.all_to_all(sent, AXES, split_axis=0, concat_axis=0, tiled=True)


def local(sky_image, coef_dual, vis_dual, visibilities, kernel_blocks, tile_rows, tile_counts):
    band_count = lax.axis_size("band")
    group_count = lax.axis_size("vis")
    band_here = lax.axis_index("band")
    group_here = lax.axis_index("vis")
    device = band_here * group_count + group_here
    kernel_here = kernel_blocks[0, 0]
    rows_here = tile_rows[0, 0]
    owners, slot_count = rows_here.shape
    rows, image_width = sky_image.shape
    stripe = image_width // band_count
    samples, length = kernel_here.shape[-2:]
    half_rows = coef_dual.shape[1]
    outer = image_width // LANES
    inner = image_width // outer
    vis_tiles = owners * slot_count
    far = group_count // 4
    tiles = min(far * vis_tiles, max(vis_tiles, 256))
    blocks_f = far * vis_tiles // tiles
    masks_x = tuple(range(1, band_count))
    masks_z = tuple(range(4, group_count, 4))

    live_slots = (
        jnp.arange(slot_count, dtype=jnp.int32)[None, :] < tile_counts[0, 0][:, None]
    ).astype(f32)[:, :, None, None]
    vis_data = visibilities[0, 0]
    vis_state = vis_dual[0, 0]

    cell = band_here * stripe + rows_here.reshape(-1)
    mirrored = cell % outer > outer // 2
    kept_cell = jnp.where(mirrored, image_width - cell, cell)
    code = (kept_cell % outer) * inner + kept_cell // outer + jnp.where(mirrored, FLAG, 0)
    told = exchanged(code.astype(f32))
    by_core = jnp.arange(2)[:, None, None, None]
    by_y = 2 * jnp.arange(2)[None, :, None, None]
    by_x = jnp.arange(band_count)[None, None, :, None]
    by_z = 4 * jnp.arange(far)[None, None, None, :]
    origin = (band_here ^ by_x) * group_count + (group_here ^ (by_core + by_y + by_z))
    chosen = origin.reshape(-1, 1) == jnp.arange(band_count * group_count)[None, :]
    codes = jnp.dot(chosen.astype(f32), told, precision=lax.Precision.HIGHEST)
    codes = jnp.round(codes).astype(jnp.int32)
    codes = codes.reshape(4 * band_count * blocks_f, 1, tiles)
    columns = codes & (FLAG - 1)

    lead = min(8, half_rows)
    coef_halo = shifted(coef_dual[:, half_rows - lead :, :], AXES, 1)

    weights = vis_state.astype(bf16)
    kernel_flat = kernel_here.reshape(vis_tiles, 2 * samples, length)
    weight_real = weights[:, :, 0].reshape(vis_tiles, samples)
    weight_imag = weights[:, :, 1].reshape(vis_tiles, samples)
    weight_pair = jnp.stack(
        [
            jnp.concatenate([weight_real, weight_imag], axis=1),
            jnp.concatenate([weight_imag, -weight_real], axis=1),
        ]
    )
    sent = jnp.einsum("nmt,ynm->ynt", kernel_flat, weight_pair, preferred_element_type=f32)
    sent = (sent * live_slots.reshape(1, vis_tiles, 1)).astype(bf16)

    def unit(steps):
        angle = (2.0 * math.pi / image_width) * (steps % image_width).astype(f32)
        return jnp.cos(angle), jnp.sin(angle)

    def turned_by(steps, axis):
        near = np.arange(rows)[:, None] * steps[None, :] % image_width * (2.0 * np.pi / image_width)
        near = near if axis else near.T
        near_cos = np.cos(near).astype(np.float32)
        near_sin = np.sin(near).astype(np.float32)
        far_cos, far_sin = unit(device * rows * jnp.expand_dims(jnp.asarray(steps, jnp.int32), 1 - axis))
        return (
            near_cos * far_cos - near_sin * far_sin,
            near_sin * far_cos + near_cos * far_sin,
        )

    wave_cos, wave_sin = turned_by(np.arange(length), 1)
    scale = 1.0 / image_width
    weight_tables = (
        *split_two(scale * jnp.concatenate([wave_cos, wave_sin], axis=0)),
        *split_two(scale * jnp.concatenate([-wave_sin, wave_cos], axis=0)),
    )
    phases_turned = turned_by(np.arange(tiles) // slot_count % owners * length, 0)
    data_parts = jnp.sum(live_slots * vis_data * vis_data, axis=(0, 1)).reshape(-1)
    phases_turned, data_parts = lax.optimization_barrier((phases_turned, data_parts))

    level = joined(sent, "vis", masks_z, 1)
    tile_real = joined(level[0], "band", masks_x)
    tile_imag = joined(level[1], "vis", (2,))
    tile_real = joined(tile_real, "vis", (2,))
    tile_imag = joined(tile_imag, "band", masks_x)
    tile_real = tile_real.reshape(2, band_count, blocks_f, tiles, length)
    tile_imag = tile_imag.reshape(band_count, 2, blocks_f, tiles, length)
    far_real = flipped(tile_real, "vis", 1)
    far_imag = flipped(tile_imag, "vis", 1)
    smooth = synthesis(coef_halo, coef_dual)

    counts = (2, band_count, blocks_f)
    large = 8 * band_count * far * vis_tiles * length * 4 > 1 << 23
    new_image, near_rows, spec_real, spec_imag, sent_real, sent_imag = image_step(
        (tile_real, tile_imag, far_real, far_imag), codes, columns, weight_tables,
        phases_turned, sky_image, smooth, bf16 if large else f32,
    )
    image_halo = shifted(near_rows, AXES, -1)
    mine_real, mine_imag = forward_parts(
        (spec_real, spec_imag), codes, columns, weight_tables, phases_turned, counts
    )
    other_real = flipped(sent_real, "vis", 1)
    other_imag = flipped(sent_imag, "vis", 1)
    step_y = band_count * blocks_f
    step_x = 2 * blocks_f

    def real_at(begin, size):
        return mine_real[begin : begin + size] + other_real[begin : begin + size]

    def imag_at(begin, size):
        return mine_imag[begin : begin + size] + other_imag[begin : begin + size]

    met_real = flipped(real_at(step_y, step_y), "vis", 2)
    met_imag = [flipped(imag_at(m * step_x, step_x), "band", m) for m in masks_x]

    def real_kept(m):
        return real_at(m * blocks_f, blocks_f) + met_real[m * blocks_f : (m + 1) * blocks_f]

    def imag_kept(y):
        span = slice(y * blocks_f, (y + 1) * blocks_f)
        return sum([met[span] for met in met_imag], imag_at(y * blocks_f, blocks_f))

    left_real = [flipped(real_kept(m), "band", m) for m in masks_x]
    left_imag = flipped(imag_kept(1), "vis", 2)
    left_real = sum(left_real, real_kept(0))
    left_imag = left_imag + imag_kept(0)
    left = jnp.stack([left_real, left_imag]).reshape(2, far, vis_tiles, length)
    seen = [flipped(left[:, 1 + index], "vis", mask) for index, mask in enumerate(masks_z)]
    seen = sum(seen, left[:, 0])

    moved_coef, abs_parts = analysis(new_image, sky_image, image_halo, coef_dual)
    totals = exchanged(
        jnp.concatenate([abs_parts[0], jnp.pad(data_parts, (0, -data_parts.size % LANES))])
    )
    data_square = jnp.sum(totals[:, LANES:])
    coef_total = jnp.sum(totals[:, :LANES])
    threshold = 0.5 * coef_total / (image_width * image_width)
    new_coef = jnp.clip(moved_coef, -threshold, threshold)

    seen = lax.reduce_precision(seen, 8, 7).astype(bf16)
    met = jnp.einsum("nmt,ynt->nym", kernel_flat, seen, preferred_element_type=f32)
    predicted = jnp.stack(
        [
            met[:, 0, :samples] - met[:, 1, samples:],
            met[:, 1, :samples] + met[:, 0, samples:],
        ],
        axis=1,
    ).reshape(vis_state.shape)
    residual = live_slots * (vis_state + predicted - vis_data)
    squares = jnp.sum(residual * residual, axis=(0, 1)).reshape(-1)
    norm_square = jnp.sum(exchanged(squares))
    radius = 0.5 * jnp.sqrt(data_square + 1e-06)
    size_value = jnp.sqrt(norm_square + 1e-06)
    new_vis = residual * (1.0 - jnp.minimum(1.0, radius / size_value))
    return (new_image, new_coef, new_vis[None, None])


def solution(mesh):
    return jax.shard_map(
        local,
        mesh=mesh,
        in_specs=(
            P(("band", "vis"), None),
            P(None, ("band", "vis"), None),
            P("band", "vis", None, None, None, None),
            P("band", "vis", None, None, None, None),
            P("band", "vis", None, None, None, None, None),
            P("band", "vis", None, None),
            P("band", "vis", None),
        ),
        out_specs=(
            P(("band", "vis"), None),
            P(None, ("band", "vis"), None),
            P("band", "vis", None, None, None, None),
        ),
        check_vma=False,
    )
```
